16 devices in a mesh: dp: 4 (over z, y), tp: 4 (over x, core).
Axes of the slice: x: 2, y: 2, z: 2, core: 2. Of those that a mesh axis runs over, the one named last changes fastest.
Arguments:
- x_in: bfloat16 [1024, 4096], P(('dp', 'tp')), parts along dimension 0
- w_in: bfloat16 [4096, 16384], P(None, 'tp')
- grad_out: bfloat16 [1024, 16384], P('dp', 'tp'), parts along dimension 0
Outputs:
- output 1: bfloat16 [1024, 4096], P(('dp', 'tp')), parts along dimension 0
- output 2: float32 [16384, 16384], P('dp', 'tp'), parts along dimension 0
There are 4 independent parts. The reference program is written for one: setup_inputs(seed, part) draws one part's arguments, and reference() takes and returns one part's arrays. A program takes and returns all parts, laid end to end along the dimension named above; an argument that names none is the same for every part.
All inputs are finite; a program needn't handle non-finite values.
Results may differ from the reference program's by a relative error of at most 0.001.
Values are sent between devices in bfloat16 or wider.
A program may use at most 1 GiB of HBM per device.

```python
import jax
import jax.numpy as jnp

TOKENS = 256
HIDDEN = 4096
FFN_DIM = 16384


def setup_inputs(seed: int = 0, part: int = 0) -> dict:
    base_key = jax.random.key(seed)
    part_key = jax.random.fold_in(base_key, part)
    key_x, key_grad = jax.random.split(part_key)
    key_weight = jax.random.key(seed + 1)
    x_in = jax.random.normal(key_x, (TOKENS, HIDDEN), jnp.float32).astype(jnp.bfloat16)
    w_in = (jax.random.normal(key_weight, (HIDDEN, FFN_DIM), jnp.float32) * HIDDEN ** -0.5).astype(jnp.bfloat16)
    grad_scale = (HIDDEN / FFN_DIM) ** 0.5
    grad_out = (jax.random.normal(key_grad, (TOKENS, FFN_DIM), jnp.float32) * grad_scale).astype(jnp.bfloat16)
    return {"x_in": x_in, "w_in": w_in, "grad_out": grad_out}


def reference(x_in, w_in, grad_out):
    grad_x = jnp.dot(grad_out, w_in.T, preferred_element_type=jnp.float32).astype(jnp.bfloat16)
    grad_w = jnp.dot(x_in.T, grad_out, preferred_element_type=jnp.float32)
    return (grad_x, grad_w)
```

```python
import functools

import jax
import jax.numpy as jnp
from jax import lax
from jax.experimental import pallas as pl
from jax.experimental.pallas import tpu as pltpu
from jax.sharding import PartitionSpec as P


MESH = pl.DeviceIdType.MESH
CROSS = [(0, 2), (1, 3), (2, 0), (3, 1)]
SIBLING = [(0, 1), (1, 0), (2, 3), (3, 2)]


def neighbours():
    me = lax.axis_index("tp")
    sib = me + 1 - 2 * lax.rem(me, 2)
    return me, lax.rem(me + 2, 4), sib, lax.rem(sib + 2, 4)


def dx_kernel(chunk, depth, g_ref, w_ref, far_ref, near_ref, g_buf, w_buf, own, send, recv, out_buf,
              g_sem, w_sem, send_sem, recv_sem, out_sem):
    order = neighbours()
    sib = order[2]
    tokens = g_ref.shape[0] // 4
    steps = w_ref.shape[0] // chunk

    def fetch_w(c):
        slot = lax.rem(c, depth)
        rows = pl.ds(pl.multiple_of(c * chunk, chunk), chunk)
        return pltpu.make_async_copy(w_ref.at[rows], w_buf.at[slot], w_sem.at[slot])

    g_copies = []
    for j, idx in enumerate(order):
        rows = pl.ds(pl.multiple_of(idx * tokens, tokens), tokens)
        g_copies.append(pltpu.make_async_copy(g_ref.at[rows], g_buf.at[pl.ds(j * tokens, tokens)], g_sem.at[j]))
        g_copies[-1].start()
    for c in range(depth):
        fetch_w(c).start()

    barrier = pltpu.get_barrier_semaphore()
    pl.semaphore_signal(barrier, inc=1, device_id={"tp": sib}, device_id_type=MESH)
    pl.semaphore_wait(barrier, 1)
    for copy in g_copies:
        copy.wait()

    def to_sibling(c):
        return pltpu.make_async_remote_copy(
            src_ref=send.at[c], dst_ref=recv.at[c], send_sem=send_sem.at[c], recv_sem=recv_sem.at[c],
            device_id={"tp": sib}, device_id_type=MESH)

    def put(c, half, ref):
        cols = pl.ds(pl.multiple_of(c * chunk, chunk), chunk)
        return pltpu.make_async_copy(
            out_buf.at[c, pl.ds(half * tokens, tokens)], ref.at[:, cols], out_sem.at[half, c])

    def finish(c):
        to_sibling(c).wait_recv()
        out_buf[c] = own[c] + recv[c]
        put(c, 1, far_ref).start()
        put(c, 0, near_ref).start()

    def step(c, carry):
        fetch_w(c).wait()
        part = lax.dot_general(g_buf[...], w_buf[lax.rem(c, depth)], (((1,), (1,)), ((), ())),
                               preferred_element_type=jnp.float32)
        own[c] = part[: 2 * tokens]
        send[c] = part[2 * tokens:]

        @pl.when(c + depth < steps)
        def _():
            fetch_w(c + depth).start()

        @pl.when(c >= 1)
        def _():
            finish(c - 1)

        to_sibling(c).start()
        return carry

    lax.fori_loop(0, steps, step, 0)
    finish(steps - 1)

    def drain(c, carry):
        to_sibling(c).wait_send()
        put(c, 0, near_ref).wait()
        put(c, 1, far_ref).wait()
        return carry

    lax.fori_loop(0, steps, drain, 0)


def dx_partial(g, w, chunk=512, depth=3):
    tokens, (hidden, ffn) = g.shape[0] // 4, w.shape
    steps = hidden // chunk
    piece = jax.ShapeDtypeStruct((tokens, hidden), jnp.float32)
    return pl.pallas_call(
        functools.partial(dx_kernel, chunk, depth),
        out_shape=(piece, piece),
        in_specs=[pl.BlockSpec(memory_space=pl.ANY)] * 2,
        out_specs=[pl.BlockSpec(memory_space=pl.ANY)] * 2,
        scratch_shapes=[
            pltpu.VMEM(g.shape, g.dtype),
            pltpu.VMEM((depth, chunk, ffn), w.dtype),
            pltpu.VMEM((steps, 2 * tokens, chunk), jnp.float32),
            pltpu.VMEM((steps, 2 * tokens, chunk), jnp.float32),
            pltpu.VMEM((steps, 2 * tokens, chunk), jnp.float32),
            pltpu.VMEM((steps, 2 * tokens, chunk), jnp.float32),
            pltpu.SemaphoreType.DMA((4,)),
            pltpu.SemaphoreType.DMA((depth,)),
            pltpu.SemaphoreType.DMA((steps,)),
            pltpu.SemaphoreType.DMA((steps,)),
            pltpu.SemaphoreType.DMA((2, steps)),
        ],
        cost_estimate=pl.CostEstimate(
            flops=2 * g.shape[0] * hidden * ffn, bytes_accessed=2 * hidden * ffn, transcendentals=0),
        compiler_params=pltpu.CompilerParams(
            collective_id=0, has_side_effects=True, vmem_limit_bytes=40 * 1024 * 1024),
        name="dx_partial",
    )(g, w)


def dw_kernel(x0, x1, x2, x3, g_ref, out_ref, x_buf):
    tokens = x0.shape[0]
    for idx, x in zip(neighbours(), (x0, x1, x2, x3)):
        x_buf[pl.ds(pl.multiple_of(idx * tokens, tokens), tokens), :] = x[...]
    out_ref[...] = lax.dot_general(x_buf[...], g_ref[...], (((0,), (0,)), ((), ())),
                                   preferred_element_type=jnp.float32)


def dw(blocks, g, rows=256):
    tokens, hidden = blocks[0].shape
    ffn = g.shape[1]
    return pl.pallas_call(
        dw_kernel,
        out_shape=jax.ShapeDtypeStruct((hidden, ffn), jnp.float32),
        grid=(hidden // rows,),
        in_specs=[pl.BlockSpec((tokens, rows), lambda i: (0, i))] * 4
        + [pl.BlockSpec(g.shape, lambda i: (0, 0))],
        out_specs=pl.BlockSpec((rows, ffn), lambda i: (i, 0)),
        scratch_shapes=[pltpu.VMEM((4 * tokens, rows), g.dtype)],
        cost_estimate=pl.CostEstimate(
            flops=8 * tokens * hidden * ffn, bytes_accessed=4 * hidden * ffn, transcendentals=0),
        compiler_params=pltpu.CompilerParams(vmem_limit_bytes=40 * 1024 * 1024),
        name="dw",
    )(*blocks, g)


def solution(mesh):
    def per_device(x, w, g):
        x_cross = lax.ppermute(x, "tp", CROSS)
        x_sib = lax.ppermute(x, "tp", SIBLING)
        far, near = dx_partial(g, w)
        arrived = lax.ppermute(far, "tp", CROSS)
        x_last = lax.ppermute(x_cross, "tp", SIBLING)
        grad_w = dw((x, x_cross, x_sib, x_last), g)
        return (near + arrived).astype(jnp.bfloat16), grad_w

    return jax.shard_map(
        per_device,
        mesh=mesh,
        in_specs=(P(("dp", "tp"), None), P(None, "tp"), P("dp", "tp")),
        out_specs=(P(("dp", "tp"), None), P("dp", "tp")),
        check_vma=False,
    )
```

```python
import jax
import jax.numpy as jnp
from jax import lax
from jax.experimental import pallas as pl
from jax.experimental.pallas import tpu as pltpu
from jax.sharding import PartitionSpec as P


MESH = pl.DeviceIdType.MESH
CROSS = [(0, 2), (1, 3), (2, 0), (3, 1)]
SIBLING = [(0, 1), (1, 0), (2, 3), (3, 2)]
CHUNK = 512


def neighbours():
    me = lax.axis_index("tp")
    sib = me + 1 - 2 * lax.rem(me, 2)
    return me, lax.rem(me + 2, 4), sib, lax.rem(sib + 2, 4)


def dx_kernel(g_ref, w_ref, far_ref, near_ref, g_buf, w_buf, own, send, recv, g_sem, w_sem, send_sem, recv_sem):
    order = neighbours()
    sib = order[2]
    tokens, ffn = g_ref.shape[0] // 4, g_ref.shape[1]
    slots, chunk = w_buf.shape[0] // CHUNK, CHUNK
    chunks = w_ref.shape[0] // chunk
    halves = (pl.ds(0, ffn // 2), pl.ds(ffn // 2, ffn // 2))

    def fetch_g(k):
        return [
            pltpu.make_async_copy(
                g_ref.at[pl.ds(pl.multiple_of(idx * tokens, tokens), tokens), halves[k]],
                g_buf.at[pl.ds(j * tokens, tokens), halves[k]], g_sem.at[j, k])
            for j, idx in enumerate(order)]

    def fetch_half(c, k):
        return pltpu.make_async_copy(
            w_ref.at[pl.ds(c * chunk, chunk), halves[k]],
            w_buf.at[pl.ds(c % slots * chunk, chunk), halves[k]], w_sem.at[c % slots, k])

    def fetch(c):
        return pltpu.make_async_copy(
            w_ref.at[pl.ds(pl.multiple_of(c * chunk, chunk), chunk)],
            w_buf.at[pl.ds(pl.multiple_of(lax.rem(c, slots) * chunk, chunk), chunk)], w_sem.at[lax.rem(c, slots), 0])

    def to_sibling(c):
        return pltpu.make_async_remote_copy(
            src_ref=send.at[c], dst_ref=recv.at[c], send_sem=send_sem.at[c], recv_sem=recv_sem.at[c],
            device_id={"tp": sib}, device_id_type=MESH)

    def product(g, w):
        return lax.dot_general(g, w, (((1,), (1,)), ((), ())), preferred_element_type=jnp.float32)

    def keep(c, part):
        own[c] = part[: 2 * tokens]
        send[c] = part[2 * tokens:]

    def finish(c):
        to_sibling(c).wait_recv()
        cols = pl.ds(pl.multiple_of(c * chunk, chunk), chunk)
        near_ref[:, cols] = own[c, :tokens] + recv[c, :tokens]
        far_ref[:, cols] = own[c, tokens:] + recv[c, tokens:]

    for k in range(2):
        for copy in fetch_g(k):
            copy.start()
        fetch_half(0, k).start()
    for c in range(1, slots):
        fetch(c).start()

    barrier = pltpu.get_barrier_semaphore()
    pl.semaphore_signal(barrier, inc=1, device_id={"tp": sib}, device_id_type=MESH)
    pl.semaphore_wait(barrier, 1)

    def by_halves(c):
        for k in range(2):
            if c == 0:
                for copy in fetch_g(k):
                    copy.wait()
            fetch_half(c, k).wait()
            part = product(g_buf[:, halves[k]], w_buf[pl.ds(c % slots * chunk, chunk), halves[k]])
            if k:
                part = part + jnp.concatenate([own[c], send[c]], axis=0)
            keep(c, part)
        to_sibling(c).start()

    by_halves(0)
    fetch(slots).start()

    def pair(i, carry):
        c = 2 * i + 1
        fetch(c).wait()
        fetch(c + 1).wait()
        rows = pl.ds(pl.multiple_of(lax.rem(c, slots) * chunk, chunk), 2 * chunk)
        part = product(g_buf[...], w_buf[rows])
        keep(c, part[:, :chunk])
        keep(c + 1, part[:, chunk:])
        for d in (0, 1):
            @pl.when(c + d + slots < chunks - 1)
            def _():
                fetch(c + d + slots).start()

        @pl.when(c + 1 + slots == chunks - 1)
        def _():
            fetch_half(chunks - 1, 0).start()
            fetch_half(chunks - 1, 1).start()

        finish(c - 1)

        @pl.when(c >= 2)
        def _():
            finish(c - 2)

        to_sibling(c).start()
        to_sibling(c + 1).start()
        return carry

    lax.fori_loop(0, (chunks - 2) // 2, pair, 0)
    by_halves(chunks - 1)
    for c in range(chunks - 3, chunks):
        finish(c)
    for c in range(chunks):
        to_sibling(c).wait_send()


def dx_partial(g, w, slots=5):
    tokens, (hidden, ffn) = g.shape[0] // 4, w.shape
    chunks = hidden // CHUNK
    piece = jax.ShapeDtypeStruct((tokens, hidden), jnp.float32)
    sums = pltpu.VMEM((chunks, 2 * tokens, CHUNK), jnp.float32)
    return pl.pallas_call(
        dx_kernel,
        out_shape=(piece, piece, jax.ShapeDtypeStruct(g.shape, g.dtype)),
        in_specs=[pl.BlockSpec(memory_space=pl.ANY)] * 2,
        out_specs=[pl.BlockSpec(memory_space=pltpu.VMEM)] * 3,
        scratch_shapes=[
            pltpu.VMEM((slots * CHUNK, ffn), w.dtype),
            sums, sums, sums,
            pltpu.SemaphoreType.DMA((4, 2)),
            pltpu.SemaphoreType.DMA((slots, 2)),
            pltpu.SemaphoreType.DMA((chunks,)),
            pltpu.SemaphoreType.DMA((chunks,)),
        ],
        cost_estimate=pl.CostEstimate(
            flops=2 * g.shape[0] * hidden * ffn, bytes_accessed=2 * hidden * ffn, transcendentals=0),
        compiler_params=pltpu.CompilerParams(
            collective_id=0, has_side_effects=True, vmem_limit_bytes=49 * 1024 * 1024),
        name="dx_partial",
    )(g, w)


def dw_kernel(x0, x1, x2, x3, g_ref, out_ref, x_buf, out_buf, out_sem):
    tokens, hidden = x0.shape
    slots, rows = out_buf.shape[0], out_buf.shape[1]
    steps = hidden // rows
    for j, x in enumerate((x0, x1, x2, x3)):
        x_buf[j * tokens:(j + 1) * tokens] = x[...]

    def put(i):
        return pltpu.make_async_copy(
            out_buf.at[lax.rem(i, slots)], out_ref.at[pl.ds(pl.multiple_of(i * rows, rows), rows)],
            out_sem.at[lax.rem(i, slots)])

    def step(i, carry):
        @pl.when(i >= slots)
        def _():
            put(i - slots).wait()

        out_buf[lax.rem(i, slots)] = lax.dot_general(
            x_buf[:, pl.ds(pl.multiple_of(i * rows, rows), rows)], g_ref[...],
            (((0,), (0,)), ((), ())), preferred_element_type=jnp.float32)
        put(i).start()
        return carry

    lax.fori_loop(0, steps, step, 0)
    for i in range(steps - slots, steps):
        put(i).wait()


def dw(blocks, g, rows=128, slots=8):
    tokens, hidden = blocks[0].shape
    ffn = g.shape[1]
    return pl.pallas_call(
        dw_kernel,
        out_shape=jax.ShapeDtypeStruct((hidden, ffn), jnp.float32),
        in_specs=[pl.BlockSpec(memory_space=pltpu.VMEM)] * 5,
        out_specs=pl.BlockSpec(memory_space=pltpu.HBM),
        scratch_shapes=[
            pltpu.VMEM((4 * tokens, hidden), g.dtype),
            pltpu.VMEM((slots, rows, ffn), jnp.float32),
            pltpu.SemaphoreType.DMA((slots,)),
        ],
        cost_estimate=pl.CostEstimate(
            flops=8 * tokens * hidden * ffn, bytes_accessed=4 * hidden * ffn, transcendentals=0),
        compiler_params=pltpu.CompilerParams(vmem_limit_bytes=40 * 1024 * 1024),
        name="dw",
    )(*blocks, g)


def solution(mesh):
    def per_device(x, w, g):
        x_cross = lax.ppermute(x, "tp", CROSS)
        x_sib = lax.ppermute(x, "tp", SIBLING)
        far, near, g_here = dx_partial(g, w)
        arrived = lax.ppermute(far, "tp", CROSS)
        x_last = lax.ppermute(x_cross, "tp", SIBLING)
        grad_w = dw((x, x_cross, x_sib, x_last), g_here)
        return (near + arrived).astype(jnp.bfloat16), grad_w

    return jax.shard_map(
        per_device,
        mesh=mesh,
        in_specs=(P(("dp", "tp"), None), P(None, "tp"), P("dp", "tp")),
        out_specs=(P(("dp", "tp"), None), P("dp", "tp")),
        check_vma=False,
    )
```

```python
import jax
import jax.numpy as jnp
from jax import lax
from jax.experimental import pallas as pl
from jax.experimental.pallas import tpu as pltpu
from jax.sharding import PartitionSpec as P


MESH = pl.DeviceIdType.MESH
CROSS = [(0, 2), (1, 3), (2, 0), (3, 1)]
CHUNK = 512
SLOTS = 5
PIECES = 4
EARLY = 1


def neighbours():
    me = lax.axis_index("tp")
    sib = me + 1 - 2 * lax.rem(me, 2)
    return me, lax.rem(me + 2, 4), sib, lax.rem(sib + 2, 4)


def front_kernel(x_ref, g_ref, w_ref, near_ref, far_ref, early_ref, x_all, g_all,
                 w_buf, own, send, recv, early_src,
                 x_sem, g_sem, w_sem, sum_send, sum_recv, sib_send, sib_recv,
                 cross_send, cross_recv, last_send, last_recv, early_send, early_recv):
    order = neighbours()
    _, cross, sib, _ = order
    tokens = x_ref.shape[0]
    chunks = w_ref.shape[0] // CHUNK
    piece = x_ref.shape[1] // PIECES

    def remote(src, dst, send_sem, recv_sem, to):
        return pltpu.make_async_remote_copy(
            src_ref=src, dst_ref=dst, send_sem=send_sem, recv_sem=recv_sem,
            device_id={"tp": to}, device_id_type=MESH)

    def block(j):
        return pl.ds(j * tokens, tokens)

    def chunk_of(c):
        return pl.ds(pl.multiple_of(c * CHUNK, CHUNK), CHUNK)

    fetch_x = pltpu.make_async_copy(x_ref, x_all.at[block(0)], x_sem)
    fetch_g = [
        pltpu.make_async_copy(
            g_ref.at[pl.ds(pl.multiple_of(idx * tokens, tokens), tokens)], g_all.at[block(j)], g_sem.at[j])
        for j, idx in enumerate(order)]

    def fetch_w(c):
        slot = lax.rem(c, SLOTS)
        return pltpu.make_async_copy(w_ref.at[chunk_of(c)], w_buf.at[slot], w_sem.at[slot])

    def cross_piece(p):
        cols = pl.ds(p * piece, piece)
        return remote(x_ref.at[:, cols], x_all.at[block(1), cols], cross_send.at[p], cross_recv.at[p], cross)

    def last_piece(p):
        cols = pl.ds(p * piece, piece)
        return remote(x_all.at[block(1), cols], x_all.at[block(3), cols], last_send.at[p], last_recv.at[p], sib)

    def to_sibling(c):
        return remote(send.at[c], recv.at[c], sum_send.at[c], sum_recv.at[c], sib)

    def early(c):
        return remote(early_src.at[c], early_ref.at[c], early_send.at[c], early_recv.at[c], cross)

    x_to_sibling = remote(x_ref, x_all.at[block(2)], sib_send, sib_recv, sib)

    for copy in fetch_g:
        copy.start()
    for c in range(SLOTS):
        fetch_w(c).start()

    barrier = pltpu.get_barrier_semaphore()
    for to in (sib, cross):
        pl.semaphore_signal(barrier, inc=1, device_id={"tp": to}, device_id_type=MESH)
    pl.semaphore_wait(barrier, 2)
    for p in range(PIECES):
        cross_piece(p).start()
    x_to_sibling.start()
    fetch_x.start()
    for copy in fetch_g:
        copy.wait()

    def forward(p):
        cross_piece(p).wait_recv()
        last_piece(p).start()

    def finish(c):
        to_sibling(c).wait_recv()
        near_ref[:, chunk_of(c)] = own[c, :tokens] + recv[c, :tokens]
        total = own[c, tokens:] + recv[c, tokens:]

        @pl.when(c < EARLY)
        def _():
            early_src[0] = total

        @pl.when(c >= EARLY)
        def _():
            far_ref[:, chunk_of(c - EARLY)] = total

    def step(c, carry):
        fetch_w(c).wait()
        part = lax.dot_general(g_all[...], w_buf[lax.rem(c, SLOTS)], (((1,), (1,)), ((), ())),
                               preferred_element_type=jnp.float32)
        own[c] = part[:2 * tokens]
        send[c] = part[2 * tokens:]

        @pl.when(c + SLOTS < chunks)
        def _():
            fetch_w(c + SLOTS).start()

        @pl.when(c >= 1)
        def _():
            finish(c - 1)

        to_sibling(c).start()
        for p in range(PIECES - 1):
            @pl.when(c == 2 * p + 2)
            def _():
                forward(p)

        @pl.when(c == 2)
        def _():
            early(0).start()

        return carry

    lax.fori_loop(0, chunks, step, 0)
    finish(chunks - 1)
    forward(PIECES - 1)
    x_to_sibling.wait()
    fetch_x.wait()
    for c in range(chunks):
        to_sibling(c).wait_send()
    for c in range(EARLY):
        early(c).wait()
    for p in range(PIECES):
        cross_piece(p).wait_send()
        last_piece(p).wait()


def front(x, g, w):
    tokens, (hidden, ffn) = x.shape[0], w.shape
    chunks = hidden // CHUNK
    dma = pltpu.SemaphoreType.DMA
    sums = pltpu.VMEM((chunks, 2 * tokens, CHUNK), jnp.float32)
    return pl.pallas_call(
        front_kernel,
        out_shape=(
            jax.ShapeDtypeStruct((tokens, hidden), jnp.float32),
            jax.ShapeDtypeStruct((tokens, hidden - EARLY * CHUNK), jnp.float32),
            jax.ShapeDtypeStruct((EARLY, tokens, CHUNK), jnp.float32),
            jax.ShapeDtypeStruct((4 * tokens, hidden), x.dtype),
            jax.ShapeDtypeStruct(g.shape, g.dtype),
        ),
        in_specs=[pl.BlockSpec(memory_space=pl.ANY)] * 3,
        out_specs=[pl.BlockSpec(memory_space=pltpu.VMEM)] * 5,
        scratch_shapes=[
            pltpu.VMEM((SLOTS, CHUNK, ffn), w.dtype),
            sums, sums, sums,
            pltpu.VMEM((EARLY, tokens, CHUNK), jnp.float32),
            dma, dma((4,)), dma((SLOTS,)), dma((chunks,)), dma((chunks,)), dma, dma,
            dma((PIECES,)), dma((PIECES,)), dma((PIECES,)), dma((PIECES,)), dma((EARLY,)), dma((EARLY,)),
        ],
        cost_estimate=pl.CostEstimate(
            flops=2 * g.shape[0] * hidden * ffn, bytes_accessed=2 * hidden * ffn, transcendentals=0),
        compiler_params=pltpu.CompilerParams(
            collective_id=0, has_side_effects=True, vmem_limit_bytes=46 * 1024 * 1024),
        name="front",
    )(x, g, w)


def dw_kernel(x_ref, g_ref, out_ref, out_buf, out_sem):
    slots, rows = out_buf.shape[0], out_buf.shape[1]
    steps = x_ref.shape[1] // rows

    def put(i):
        return pltpu.make_async_copy(
            out_buf.at[lax.rem(i, slots)], out_ref.at[pl.ds(pl.multiple_of(i * rows, rows), rows)],
            out_sem.at[lax.rem(i, slots)])

    def step(i, carry):
        @pl.when(i >= slots)
        def _():
            put(i - slots).wait()

        out_buf[lax.rem(i, slots)] = lax.dot_general(
            x_ref[:, pl.ds(pl.multiple_of(i * rows, rows), rows)], g_ref[...],
            (((0,), (0,)), ((), ())), preferred_element_type=jnp.float32)
        put(i).start()
        return carry

    lax.fori_loop(0, steps, step, 0)
    for i in range(steps - slots, steps):
        put(i).wait()


def dw(x, g, rows=128, slots=8):
    tokens, hidden = x.shape
    ffn = g.shape[1]
    return pl.pallas_call(
        dw_kernel,
        out_shape=jax.ShapeDtypeStruct((hidden, ffn), jnp.float32),
        in_specs=[pl.BlockSpec(memory_space=pltpu.VMEM)] * 2,
        out_specs=pl.BlockSpec(memory_space=pl.ANY),
        scratch_shapes=[
            pltpu.VMEM((slots, rows, ffn), jnp.float32),
            pltpu.SemaphoreType.DMA((slots,)),
        ],
        cost_estimate=pl.CostEstimate(
            flops=2 * tokens * hidden * ffn, bytes_accessed=4 * hidden * ffn, transcendentals=0),
        compiler_params=pltpu.CompilerParams(vmem_limit_bytes=40 * 1024 * 1024),
        name="dw",
    )(x, g)


def solution(mesh):
    def per_device(x, w, g):
        near, far, early, x_all, g_all = front(x, g, w)
        arrived = lax.ppermute(far, "tp", CROSS)
        grad_w = dw(x_all, g_all)
        arrived = jnp.concatenate([early[c] for c in range(EARLY)] + [arrived], axis=1)
        return (near + arrived).astype(jnp.bfloat16), grad_w

    return jax.shard_map(
        per_device,
        mesh=mesh,
        in_specs=(P(("dp", "tp"), None), P(None, "tp"), P("dp", "tp")),
        out_specs=(P(("dp", "tp"), None), P("dp", "tp")),
        check_vma=False,
    )
```

```python
import jax
import jax.numpy as jnp
from jax import lax
from jax.experimental import pallas as pl
from jax.experimental.pallas import tpu as pltpu
from jax.sharding import PartitionSpec as P


MESH = pl.DeviceIdType.MESH
CROSS = [(0, 2), (1, 3), (2, 0), (3, 1)]
CHUNK = 512
SLOTS = 3
PIECES = 4
EARLY = 1


def neighbours():
    me = lax.axis_index("tp")
    sib = me + 1 - 2 * lax.rem(me, 2)
    return me, lax.rem(me + 2, 4), sib, lax.rem(sib + 2, 4)


def front_kernel(x_ref, g_ref, w_ref, near_ref, far_ref, early_ref, x_all, g_all,
                 w_buf, own, send, recv, early_src,
                 x_sem, g_sem, w_sem, sum_send, sum_recv, sib_send, sib_recv,
                 cross_send, cross_recv, last_send, last_recv, early_send, early_recv):
    order = neighbours()
    _, cross, sib, _ = order
    tokens = x_ref.shape[0]
    chunks = w_ref.shape[0] // CHUNK
    piece = x_ref.shape[1] // PIECES

    def remote(src, dst, send_sem, recv_sem, to):
        return pltpu.make_async_remote_copy(
            src_ref=src, dst_ref=dst, send_sem=send_sem, recv_sem=recv_sem,
            device_id={"tp": to}, device_id_type=MESH)

    def block(j):
        return pl.ds(j * tokens, tokens)

    def chunk_of(c):
        return pl.ds(pl.multiple_of(c * CHUNK, CHUNK), CHUNK)

    fetch_x = pltpu.make_async_copy(x_ref, x_all.at[block(0)], x_sem)
    fetch_g = [
        pltpu.make_async_copy(
            g_ref.at[pl.ds(pl.multiple_of(idx * tokens, tokens), tokens)], g_all.at[block(j)], g_sem.at[j])
        for j, idx in enumerate(order)]

    def fetch_w(c):
        slot = lax.rem(c, SLOTS)
        return pltpu.make_async_copy(w_ref.at[chunk_of(c)], w_buf.at[slot], w_sem.at[slot])

    def cross_piece(p):
        cols = pl.ds(p * piece, piece)
        return remote(x_ref.at[:, cols], x_all.at[block(1), cols], cross_send.at[p], cross_recv.at[p], cross)

    def last_piece(p):
        cols = pl.ds(p * piece, piece)
        return remote(x_all.at[block(1), cols], x_all.at[block(3), cols], last_send.at[p], last_recv.at[p], sib)

    def to_sibling(c):
        return remote(send.at[c], recv.at[c], sum_send.at[c], sum_recv.at[c], sib)

    def early(c):
        return remote(early_src.at[c], early_ref.at[c], early_send.at[c], early_recv.at[c], cross)

    x_to_sibling = remote(x_ref, x_all.at[block(2)], sib_send, sib_recv, sib)

    barrier = pltpu.get_barrier_semaphore()
    for to in (sib, cross):
        pl.semaphore_signal(barrier, inc=1, device_id={"tp": to}, device_id_type=MESH)
    pl.semaphore_wait(barrier, 2)
    for p in range(PIECES):
        cross_piece(p).start()
    x_to_sibling.start()
    for copy in fetch_g:
        copy.start()
    for c in range(2):
        fetch_w(c).start()
    fetch_x.start()
    for copy in fetch_g:
        copy.wait()

    def forward(p):
        cross_piece(p).wait_recv()
        last_piece(p).start()

    def finish(c):
        to_sibling(c).wait_recv()
        near_ref[:, chunk_of(c)] = own[c, :tokens] + recv[c, :tokens]
        total = own[c, tokens:] + recv[c, tokens:]

        @pl.when(c < EARLY)
        def _():
            early_src[0] = total

        @pl.when(c >= EARLY)
        def _():
            far_ref[:, chunk_of(c - EARLY)] = total

    def step(c, carry):
        fetch_w(c).wait()

        @pl.when(c + 2 < chunks)
        def _():
            fetch_w(c + 2).start()

        part = lax.dot_general(g_all[...], w_buf[lax.rem(c, SLOTS)], (((1,), (1,)), ((), ())),
                               preferred_element_type=jnp.float32)
        own[c] = part[:2 * tokens]
        send[c] = part[2 * tokens:]

        @pl.when(c >= 1)
        def _():
            finish(c - 1)

        to_sibling(c).start()
        for p in range(PIECES - 1):
            @pl.when(c == 2 * p + 2)
            def _():
                forward(p)

        @pl.when(c == 2)
        def _():
            early(0).start()

        return carry

    lax.fori_loop(0, chunks, step, 0)
    finish(chunks - 1)
    forward(PIECES - 1)
    x_to_sibling.wait()
    fetch_x.wait()
    for c in range(chunks):
        to_sibling(c).wait_send()
    for c in range(EARLY):
        early(c).wait()
    for p in range(PIECES):
        cross_piece(p).wait_send()
        last_piece(p).wait()


def front(x, g, w):
    tokens, (hidden, ffn) = x.shape[0], w.shape
    chunks = hidden // CHUNK
    dma = pltpu.SemaphoreType.DMA
    sums = pltpu.VMEM((chunks, 2 * tokens, CHUNK), jnp.float32)
    return pl.pallas_call(
        front_kernel,
        out_shape=(
            jax.ShapeDtypeStruct((tokens, hidden), jnp.float32),
            jax.ShapeDtypeStruct((tokens, hidden - EARLY * CHUNK), jnp.float32),
            jax.ShapeDtypeStruct((EARLY, tokens, CHUNK), jnp.float32),
            jax.ShapeDtypeStruct((4 * tokens, hidden), x.dtype),
            jax.ShapeDtypeStruct(g.shape, g.dtype),
        ),
        in_specs=[pl.BlockSpec(memory_space=pl.ANY)] * 3,
        out_specs=[pl.BlockSpec(memory_space=pltpu.VMEM)] * 5,
        scratch_shapes=[
            pltpu.VMEM((SLOTS, CHUNK, ffn), w.dtype),
            sums, sums, sums,
            pltpu.VMEM((EARLY, tokens, CHUNK), jnp.float32),
            dma, dma((4,)), dma((SLOTS,)), dma((chunks,)), dma((chunks,)), dma, dma,
            dma((PIECES,)), dma((PIECES,)), dma((PIECES,)), dma((PIECES,)), dma((EARLY,)), dma((EARLY,)),
        ],
        cost_estimate=pl.CostEstimate(
            flops=2 * g.shape[0] * hidden * ffn, bytes_accessed=2 * hidden * ffn, transcendentals=0),
        compiler_params=pltpu.CompilerParams(
            collective_id=0, has_side_effects=True, vmem_limit_bytes=46 * 1024 * 1024),
        name="front",
    )(x, g, w)


def dw_kernel(x_ref, g_ref, out_ref, out_buf, out_sem):
    slots, rows = out_buf.shape[0], out_buf.shape[1]
    steps = x_ref.shape[1] // rows

    def put(i):
        return pltpu.make_async_copy(
            out_buf.at[lax.rem(i, slots)], out_ref.at[pl.ds(pl.multiple_of(i * rows, rows), rows)],
            out_sem.at[lax.rem(i, slots)])

    def step(i, carry):
        @pl.when(i >= slots)
        def _():
            put(i - slots).wait()

        out_buf[lax.rem(i, slots)] = lax.dot_general(
            x_ref[:, pl.ds(pl.multiple_of(i * rows, rows), rows)], g_ref[...],
            (((0,), (0,)), ((), ())), preferred_element_type=jnp.float32)
        put(i).start()
        return carry

    lax.fori_loop(0, steps, step, 0)
    for i in range(steps - slots, steps):
        put(i).wait()


def dw(x, g, rows=128, slots=8):
    tokens, hidden = x.shape
    ffn = g.shape[1]
    return pl.pallas_call(
        dw_kernel,
        out_shape=jax.ShapeDtypeStruct((hidden, ffn), jnp.float32),
        in_specs=[pl.BlockSpec(memory_space=pltpu.VMEM)] * 2,
        out_specs=pl.BlockSpec(memory_space=pl.ANY),
        scratch_shapes=[
            pltpu.VMEM((slots, rows, ffn), jnp.float32),
            pltpu.SemaphoreType.DMA((slots,)),
        ],
        cost_estimate=pl.CostEstimate(
            flops=2 * tokens * hidden * ffn, bytes_accessed=4 * hidden * ffn, transcendentals=0),
        compiler_params=pltpu.CompilerParams(vmem_limit_bytes=40 * 1024 * 1024),
        name="dw",
    )(x, g)


def solution(mesh):
    def per_device(x, w, g):
        near, far, early, x_all, g_all = front(x, g, w)
        arrived = lax.ppermute(far, "tp", CROSS)
        grad_w = dw(x_all, g_all)
        arrived = jnp.concatenate([early[c] for c in range(EARLY)] + [arrived], axis=1)
        return (near + arrived).astype(jnp.bfloat16), grad_w

    return jax.shard_map(
        per_device,
        mesh=mesh,
        in_specs=(P(("dp", "tp"), None), P(None, "tp"), P("dp", "tp")),
        out_specs=(P(("dp", "tp"), None), P("dp", "tp")),
        check_vma=False,
    )
```

```python
import jax
import jax.numpy as jnp
from jax import lax
from jax.experimental import pallas as pl
from jax.experimental.pallas import tpu as pltpu
from jax.sharding import PartitionSpec as P


MESH = pl.DeviceIdType.MESH
CROSS = [(0, 2), (1, 3), (2, 0), (3, 1)]
SIBLING = [(0, 1), (1, 0), (2, 3), (3, 2)]
CHUNK = 512
SLOTS = 3
EARLY = 256


def neighbours():
    me = lax.axis_index("tp")
    sib = me + 1 - 2 * lax.rem(me, 2)
    return me, lax.rem(me + 2, 4), sib, lax.rem(sib + 2, 4)


def front_kernel(g_ref, w_ref, near_ref, far_ref, early_ref, g_all, w_buf, own, send, recv, early_src,
                 g_sem, w_sem, sum_send, sum_recv, early_sem):
    order = neighbours()
    _, cross, sib, _ = order
    tokens = g_ref.shape[0] // 4
    chunks = w_ref.shape[0] // CHUNK

    def remote(src, dst, send_sem, recv_sem, to):
        return pltpu.make_async_remote_copy(
            src_ref=src, dst_ref=dst, send_sem=send_sem, recv_sem=recv_sem,
            device_id={"tp": to}, device_id_type=MESH)

    def chunk_of(c):
        return pl.ds(pl.multiple_of(c * CHUNK, CHUNK), CHUNK)

    fetch_g = [
        pltpu.make_async_copy(
            g_ref.at[pl.ds(pl.multiple_of(idx * tokens, tokens), tokens)],
            g_all.at[pl.ds(j * tokens, tokens)], g_sem.at[j])
        for j, idx in enumerate(order)]

    def fetch_w(c):
        slot = lax.rem(c, SLOTS)
        return pltpu.make_async_copy(w_ref.at[chunk_of(c)], w_buf.at[slot], w_sem.at[slot])

    def to_sibling(c):
        return remote(send.at[c], recv.at[c], sum_send.at[c], sum_recv.at[c], sib)

    early = remote(early_src, early_ref, early_sem.at[0], early_sem.at[1], cross)

    for copy in fetch_g:
        copy.start()
    for c in range(2):
        fetch_w(c).start()
    barrier = pltpu.get_barrier_semaphore()
    for to in (sib, cross):
        pl.semaphore_signal(barrier, inc=1, device_id={"tp": to}, device_id_type=MESH)
    pl.semaphore_wait(barrier, 2)
    for copy in fetch_g:
        copy.wait()

    def finish(c):
        to_sibling(c).wait_recv()
        near_ref[:, chunk_of(c)] = own[c, :tokens] + recv[c, :tokens]
        total = own[c, tokens:] + recv[c, tokens:]

        @pl.when(c == 0)
        def _():
            early_src[...] = total[:, :EARLY]
            far_ref[:, :CHUNK - EARLY] = total[:, EARLY:]

        @pl.when(c >= 1)
        def _():
            far_ref[:, pl.ds(pl.multiple_of(c * CHUNK - EARLY, 128), CHUNK)] = total

    def step(c, carry):
        fetch_w(c).wait()

        @pl.when(c + 2 < chunks)
        def _():
            fetch_w(c + 2).start()

        part = lax.dot_general(g_all[...], w_buf[lax.rem(c, SLOTS)], (((1,), (1,)), ((), ())),
                               preferred_element_type=jnp.float32)
        own[c] = part[:2 * tokens]
        send[c] = part[2 * tokens:]

        @pl.when(c == 2)
        def _():
            early.start()

        @pl.when(c >= 1)
        def _():
            finish(c - 1)

        to_sibling(c).start()
        return carry

    lax.fori_loop(0, chunks, step, 0)
    finish(chunks - 1)
    early.wait()
    for c in range(chunks):
        to_sibling(c).wait_send()


def front(g, w):
    tokens, (hidden, ffn) = g.shape[0] // 4, w.shape
    chunks = hidden // CHUNK
    dma = pltpu.SemaphoreType.DMA
    piece = jax.ShapeDtypeStruct((tokens, hidden), jnp.float32)
    sums = pltpu.VMEM((chunks, 2 * tokens, CHUNK), jnp.float32)
    return pl.pallas_call(
        front_kernel,
        out_shape=(piece, jax.ShapeDtypeStruct((tokens, hidden - EARLY), jnp.float32), jax.ShapeDtypeStruct((tokens, EARLY), jnp.float32),
                   jax.ShapeDtypeStruct(g.shape, g.dtype)),
        in_specs=[pl.BlockSpec(memory_space=pl.ANY)] * 2,
        out_specs=[pl.BlockSpec(memory_space=pltpu.VMEM)] * 4,
        scratch_shapes=[
            pltpu.VMEM((SLOTS, CHUNK, ffn), w.dtype),
            sums, sums, sums,
            pltpu.VMEM((tokens, EARLY), jnp.float32),
            dma((4,)), dma((SLOTS,)), dma((chunks,)), dma((chunks,)), dma((2,)),
        ],
        cost_estimate=pl.CostEstimate(
            flops=2 * g.shape[0] * hidden * ffn, bytes_accessed=2 * hidden * ffn, transcendentals=0),
        compiler_params=pltpu.CompilerParams(
            collective_id=0, has_side_effects=True, vmem_limit_bytes=48 * 1024 * 1024),
        name="front",
    )(g, w)


def dw_kernel(x0, x1, x2, x3, g_ref, out_ref, out_buf, out_sem):
    slots, rows = out_buf.shape[0], out_buf.shape[1]
    steps = x0.shape[1] // rows

    def put(i):
        return pltpu.make_async_copy(
            out_buf.at[lax.rem(i, slots)], out_ref.at[pl.ds(pl.multiple_of(i * rows, rows), rows)],
            out_sem.at[lax.rem(i, slots)])

    def step(i, carry):
        @pl.when(i >= slots)
        def _():
            put(i - slots).wait()

        cols = pl.ds(pl.multiple_of(i * rows, rows), rows)
        x = jnp.concatenate([b[:, cols] for b in (x0, x1, x2, x3)], axis=0)
        out_buf[lax.rem(i, slots)] = lax.dot_general(
            x, g_ref[...], (((0,), (0,)), ((), ())), preferred_element_type=jnp.float32)
        put(i).start()
        return carry

    lax.fori_loop(0, steps, step, 0)
    for i in range(steps - slots, steps):
        put(i).wait()


def dw(blocks, g, rows=128, slots=8):
    tokens, hidden = g.shape[0], blocks[0].shape[1]
    ffn = g.shape[1]
    return pl.pallas_call(
        dw_kernel,
        out_shape=jax.ShapeDtypeStruct((hidden, ffn), jnp.float32),
        in_specs=[pl.BlockSpec(memory_space=pltpu.VMEM)] * 5,
        out_specs=pl.BlockSpec(memory_space=pl.ANY),
        scratch_shapes=[
            pltpu.VMEM((slots, rows, ffn), jnp.float32),
            pltpu.SemaphoreType.DMA((slots,)),
        ],
        cost_estimate=pl.CostEstimate(
            flops=2 * tokens * hidden * ffn, bytes_accessed=4 * hidden * ffn, transcendentals=0),
        compiler_params=pltpu.CompilerParams(vmem_limit_bytes=40 * 1024 * 1024),
        name="dw",
    )(*blocks, g)


def solution(mesh):
    def per_device(x, w, g):
        x_cross = lax.ppermute(x, "tp", CROSS)
        x_sib = lax.ppermute(x, "tp", SIBLING)
        near, far, early, g_all = front(g, w)
        arrived = lax.ppermute(far, "tp", CROSS)
        x_last = lax.ppermute(x_cross, "tp", SIBLING)
        grad_w = dw((x, x_cross, x_sib, x_last), g_all)
        arrived = jnp.concatenate([early, arrived], axis=1)
        return (near + arrived).astype(jnp.bfloat16), grad_w

    return jax.shard_map(
        per_device,
        mesh=mesh,
        in_specs=(P(("dp", "tp"), None), P(None, "tp"), P("dp", "tp")),
        out_specs=(P(("dp", "tp"), None), P("dp", "tp")),
        check_vma=False,
    )
```

```python
import jax
import jax.numpy as jnp
from jax import lax
from jax.experimental import pallas as pl
from jax.experimental.pallas import tpu as pltpu
from jax.sharding import PartitionSpec as P


MESH = pl.DeviceIdType.MESH
CROSS = [(0, 2), (1, 3), (2, 0), (3, 1)]
CHUNK = 512
SLOTS = 3
PIECES = 4
EARLY = 256


def neighbours():
    me = lax.axis_index("tp")
    sib = me + 1 - 2 * lax.rem(me, 2)
    return me, lax.rem(me + 2, 4), sib, lax.rem(sib + 2, 4)


def front_kernel(x_ref, g_ref, w_ref, near_ref, far_ref, early_ref, x_all, g_all,
                 w_buf, own, send, recv, early_src,
                 x_sem, g_sem, w_sem, sum_send, sum_recv, sib_send, sib_recv,
                 cross_send, cross_recv, last_send, last_recv, early_send, early_recv):
    order = neighbours()
    _, cross, sib, _ = order
    tokens = x_ref.shape[0]
    chunks = w_ref.shape[0] // CHUNK
    piece = x_ref.shape[1] // PIECES

    def remote(src, dst, send_sem, recv_sem, to):
        return pltpu.make_async_remote_copy(
            src_ref=src, dst_ref=dst, send_sem=send_sem, recv_sem=recv_sem,
            device_id={"tp": to}, device_id_type=MESH)

    def block(j):
        return pl.ds(j * tokens, tokens)

    def chunk_of(c):
        return pl.ds(pl.multiple_of(c * CHUNK, CHUNK), CHUNK)

    fetch_x = pltpu.make_async_copy(x_ref, x_all.at[block(0)], x_sem)
    fetch_g = [
        pltpu.make_async_copy(
            g_ref.at[pl.ds(pl.multiple_of(idx * tokens, tokens), tokens)], g_all.at[block(j)], g_sem.at[j])
        for j, idx in enumerate(order)]

    def fetch_w(c):
        slot = lax.rem(c, SLOTS)
        return pltpu.make_async_copy(w_ref.at[chunk_of(c)], w_buf.at[slot], w_sem.at[slot])

    def cross_piece(p):
        cols = pl.ds(p * piece, piece)
        return remote(x_ref.at[:, cols], x_all.at[block(1), cols], cross_send.at[p], cross_recv.at[p], cross)

    def last_piece(p):
        cols = pl.ds(p * piece, piece)
        return remote(x_all.at[block(1), cols], x_all.at[block(3), cols], last_send.at[p], last_recv.at[p], sib)

    def to_sibling(c):
        return remote(send.at[c], recv.at[c], sum_send.at[c], sum_recv.at[c], sib)

    early = remote(early_src, early_ref, early_send, early_recv, cross)
    x_to_sibling = remote(x_ref, x_all.at[block(2)], sib_send, sib_recv, sib)

    def first_reads():
        for copy in fetch_g:
            copy.start()
        fetch_w(0).start()

    upper = order[0] >= 2

    @pl.when(jnp.logical_not(upper))
    def _():
        first_reads()

    barrier = pltpu.get_barrier_semaphore()
    for to in (sib, cross):
        pl.semaphore_signal(barrier, inc=1, device_id={"tp": to}, device_id_type=MESH)
    pl.semaphore_wait(barrier, 2)
    for p in range(PIECES):
        cross_piece(p).start()
    x_to_sibling.start()

    @pl.when(upper)
    def _():
        first_reads()

    fetch_w(1).start()
    fetch_x.start()
    for copy in fetch_g:
        copy.wait()

    def forward(p):
        cross_piece(p).wait_recv()
        last_piece(p).start()

    def finish(c):
        to_sibling(c).wait_recv()
        near_ref[:, chunk_of(c)] = own[c, :tokens] + recv[c, :tokens]
        total = own[c, tokens:] + recv[c, tokens:]

        @pl.when(c == 0)
        def _():
            early_src[...] = total[:, :EARLY]
            far_ref[:, :CHUNK - EARLY] = total[:, EARLY:]

        @pl.when(c >= 1)
        def _():
            far_ref[:, pl.ds(pl.multiple_of(c * CHUNK - EARLY, 128), CHUNK)] = total

    def step(c, carry):
        fetch_w(c).wait()

        @pl.when(c + 2 < chunks)
        def _():
            fetch_w(c + 2).start()

        part = lax.dot_general(g_all[...], w_buf[lax.rem(c, SLOTS)], (((1,), (1,)), ((), ())),
                               preferred_element_type=jnp.float32)
        own[c] = part[:2 * tokens]
        send[c] = part[2 * tokens:]

        @pl.when(c >= 1)
        def _():
            finish(c - 1)

        to_sibling(c).start()
        for p in range(PIECES - 1):
            @pl.when(c == 2 * p + 2)
            def _():
                forward(p)

        @pl.when(c == 2)
        def _():
            early.start()

        return carry

    lax.fori_loop(0, chunks, step, 0)
    finish(chunks - 1)
    forward(PIECES - 1)
    x_to_sibling.wait()
    fetch_x.wait()
    for c in range(chunks):
        to_sibling(c).wait_send()
    early.wait()
    for p in range(PIECES):
        cross_piece(p).wait_send()
        last_piece(p).wait()


def front(x, g, w):
    tokens, (hidden, ffn) = x.shape[0], w.shape
    chunks = hidden // CHUNK
    dma = pltpu.SemaphoreType.DMA
    sums = pltpu.VMEM((chunks, 2 * tokens, CHUNK), jnp.float32)
    return pl.pallas_call(
        front_kernel,
        out_shape=(
            jax.ShapeDtypeStruct((tokens, hidden), jnp.float32),
            jax.ShapeDtypeStruct((tokens, hidden - EARLY), jnp.float32),
            jax.ShapeDtypeStruct((tokens, EARLY), jnp.float32),
            jax.ShapeDtypeStruct((4 * tokens, hidden), x.dtype),
            jax.ShapeDtypeStruct(g.shape, g.dtype),
        ),
        in_specs=[pl.BlockSpec(memory_space=pl.ANY)] * 3,
        out_specs=[pl.BlockSpec(memory_space=pltpu.VMEM)] * 5,
        scratch_shapes=[
            pltpu.VMEM((SLOTS, CHUNK, ffn), w.dtype),
            sums, sums, sums,
            pltpu.VMEM((tokens, EARLY), jnp.float32),
            dma, dma((4,)), dma((SLOTS,)), dma((chunks,)), dma((chunks,)), dma, dma,
            dma((PIECES,)), dma((PIECES,)), dma((PIECES,)), dma((PIECES,)), dma, dma,
        ],
        cost_estimate=pl.CostEstimate(
            flops=2 * g.shape[0] * hidden * ffn, bytes_accessed=2 * hidden * ffn, transcendentals=0),
        compiler_params=pltpu.CompilerParams(
            collective_id=0, has_side_effects=True, vmem_limit_bytes=46 * 1024 * 1024),
        name="front",
    )(x, g, w)


def dw_kernel(x_ref, g_ref, out_ref, out_buf, out_sem):
    slots, rows = out_buf.shape[0], out_buf.shape[1]
    steps = x_ref.shape[1] // rows

    def put(i):
        return pltpu.make_async_copy(
            out_buf.at[lax.rem(i, slots)], out_ref.at[pl.ds(pl.multiple_of(i * rows, rows), rows)],
            out_sem.at[lax.rem(i, slots)])

    def step(i, carry):
        @pl.when(i >= slots)
        def _():
            put(i - slots).wait()

        out_buf[lax.rem(i, slots)] = lax.dot_general(
            x_ref[:, pl.ds(pl.multiple_of(i * rows, rows), rows)], g_ref[...],
            (((0,), (0,)), ((), ())), preferred_element_type=jnp.float32)
        put(i).start()
        return carry

    lax.fori_loop(0, steps, step, 0)
    for i in range(steps - slots, steps):
        put(i).wait()


def dw(x, g, rows=128, slots=8):
    tokens, hidden = x.shape
    ffn = g.shape[1]
    return pl.pallas_call(
        dw_kernel,
        out_shape=jax.ShapeDtypeStruct((hidden, ffn), jnp.float32),
        in_specs=[pl.BlockSpec(memory_space=pltpu.VMEM)] * 2,
        out_specs=pl.BlockSpec(memory_space=pl.ANY),
        scratch_shapes=[
            pltpu.VMEM((slots, rows, ffn), jnp.float32),
            pltpu.SemaphoreType.DMA((slots,)),
        ],
        cost_estimate=pl.CostEstimate(
            flops=2 * tokens * hidden * ffn, bytes_accessed=4 * hidden * ffn, transcendentals=0),
        compiler_params=pltpu.CompilerParams(vmem_limit_bytes=40 * 1024 * 1024),
        name="dw",
    )(x, g)


def solution(mesh):
    def per_device(x, w, g):
        near, far, early, x_all, g_all = front(x, g, w)
        arrived = lax.ppermute(far, "tp", CROSS)
        grad_w = dw(x_all, g_all)
        arrived = jnp.concatenate([early, arrived], axis=1)
        return (near + arrived).astype(jnp.bfloat16), grad_w

    return jax.shard_map(
        per_device,
        mesh=mesh,
        in_specs=(P(("dp", "tp"), None), P(None, "tp"), P("dp", "tp")),
        out_specs=(P(("dp", "tp"), None), P("dp", "tp")),
        check_vma=False,
    )
```

```python
import jax
import jax.numpy as jnp
from jax import lax
from jax.experimental import pallas as pl
from jax.experimental.pallas import tpu as pltpu
from jax.sharding import PartitionSpec as P


MESH = pl.DeviceIdType.MESH
CROSS = [(0, 2), (1, 3), (2, 0), (3, 1)]
CHUNK = 512
SLOTS = 3
PIECES = 4
EARLY = 256


def neighbours():
    me = lax.axis_index("tp")
    sib = me + 1 - 2 * lax.rem(me, 2)
    return me, lax.rem(me + 2, 4), sib, lax.rem(sib + 2, 4)


def front_kernel(x_ref, g_ref, w_ref, near_ref, far_ref, early_ref, x_all, g_all,
                 w_buf, own, send, recv, early_src,
                 x_sem, g_sem, w_sem, sum_send, sum_recv, sib_send, sib_recv,
                 cross_send, cross_recv, last_send, last_recv, early_send, early_recv):
    order = neighbours()
    _, cross, sib, _ = order
    tokens = x_ref.shape[0]
    chunks = w_ref.shape[0] // CHUNK
    piece = x_ref.shape[1] // PIECES

    def remote(src, dst, send_sem, recv_sem, to):
        return pltpu.make_async_remote_copy(
            src_ref=src, dst_ref=dst, send_sem=send_sem, recv_sem=recv_sem,
            device_id={"tp": to}, device_id_type=MESH)

    def block(j):
        return pl.ds(j * tokens, tokens)

    def chunk_of(c):
        return pl.ds(pl.multiple_of(c * CHUNK, CHUNK), CHUNK)

    fetch_x = pltpu.make_async_copy(x_ref, x_all.at[block(0)], x_sem)
    fetch_g = [
        pltpu.make_async_copy(
            g_ref.at[pl.ds(pl.multiple_of(idx * tokens, tokens), tokens)], g_all.at[block(j)], g_sem.at[j])
        for j, idx in enumerate(order)]

    def fetch_w(c):
        slot = lax.rem(c, SLOTS)
        return pltpu.make_async_copy(w_ref.at[chunk_of(c)], w_buf.at[slot], w_sem.at[slot])

    def cross_piece(p):
        cols = pl.ds(p * piece, piece)
        return remote(x_ref.at[:, cols], x_all.at[block(1), cols], cross_send.at[p], cross_recv.at[p], cross)

    def last_piece(p):
        cols = pl.ds(p * piece, piece)
        return remote(x_all.at[block(1), cols], x_all.at[block(3), cols], last_send.at[p], last_recv.at[p], sib)

    def to_sibling(c):
        return remote(send.at[c], recv.at[c], sum_send.at[c], sum_recv.at[c], sib)

    early = remote(early_src, early_ref, early_send, early_recv, cross)
    x_to_sibling = remote(x_ref, x_all.at[block(2)], sib_send, sib_recv, sib)

    def first_reads():
        for copy in fetch_g:
            copy.start()
        fetch_w(0).start()

    upper = order[0] >= 2

    @pl.when(jnp.logical_not(upper))
    def _():
        first_reads()

    barrier = pltpu.get_barrier_semaphore()
    for to in (sib, cross):
        pl.semaphore_signal(barrier, inc=1, device_id={"tp": to}, device_id_type=MESH)
    pl.semaphore_wait(barrier, 2)
    for p in range(PIECES):
        cross_piece(p).start()
    x_to_sibling.start()

    @pl.when(upper)
    def _():
        first_reads()

    fetch_w(1).start()
    fetch_x.start()
    for copy in fetch_g:
        copy.wait()

    def forward(p):
        cross_piece(p).wait_recv()
        last_piece(p).start()

    def finish(c):
        to_sibling(c).wait_recv()
        near_ref[:, chunk_of(c)] = own[c, :tokens] + recv[c, :tokens]
        total = own[c, tokens:] + recv[c, tokens:]

        @pl.when(c == 0)
        def _():
            early_src[...] = total[:, :EARLY]
            far_ref[:, :CHUNK - EARLY] = total[:, EARLY:]

        @pl.when(c >= 1)
        def _():
            far_ref[:, pl.ds(pl.multiple_of(c * CHUNK - EARLY, 128), CHUNK)] = total

    def step(c, carry):
        fetch_w(c).wait()

        @pl.when(c + 2 < chunks)
        def _():
            fetch_w(c + 2).start()

        part = lax.dot_general(g_all[...], w_buf[lax.rem(c, SLOTS)], (((1,), (1,)), ((), ())),
                               preferred_element_type=jnp.float32)
        own[c] = part[:2 * tokens]
        send[c] = part[2 * tokens:]

        @pl.when(c >= 1)
        def _():
            finish(c - 1)

        to_sibling(c).start()
        for p, when in enumerate((2, 4, 6, 7)):
            @pl.when(c == when)
            def _():
                forward(p)

        @pl.when(c == 2)
        def _():
            early.start()

        return carry

    lax.fori_loop(0, chunks, step, 0)
    finish(chunks - 1)
    x_to_sibling.wait()
    fetch_x.wait()
    for c in range(chunks):
        to_sibling(c).wait_send()
    early.wait()
    for p in range(PIECES):
        cross_piece(p).wait_send()
        last_piece(p).wait()


def front(x, g, w):
    tokens, (hidden, ffn) = x.shape[0], w.shape
    chunks = hidden // CHUNK
    dma = pltpu.SemaphoreType.DMA
    sums = pltpu.VMEM((chunks, 2 * tokens, CHUNK), jnp.float32)
    return pl.pallas_call(
        front_kernel,
        out_shape=(
            jax.ShapeDtypeStruct((tokens, hidden), jnp.float32),
            jax.ShapeDtypeStruct((tokens, hidden - EARLY), jnp.float32),
            jax.ShapeDtypeStruct((tokens, EARLY), jnp.float32),
            jax.ShapeDtypeStruct((4 * tokens, hidden), x.dtype),
            jax.ShapeDtypeStruct(g.shape, g.dtype),
        ),
        in_specs=[pl.BlockSpec(memory_space=pl.ANY)] * 3,
        out_specs=[pl.BlockSpec(memory_space=pltpu.VMEM)] * 5,
        scratch_shapes=[
            pltpu.VMEM((SLOTS, CHUNK, ffn), w.dtype),
            sums, sums, sums,
            pltpu.VMEM((tokens, EARLY), jnp.float32),
            dma, dma((4,)), dma((SLOTS,)), dma((chunks,)), dma((chunks,)), dma, dma,
            dma((PIECES,)), dma((PIECES,)), dma((PIECES,)), dma((PIECES,)), dma, dma,
        ],
        cost_estimate=pl.CostEstimate(
            flops=2 * g.shape[0] * hidden * ffn, bytes_accessed=2 * hidden * ffn, transcendentals=0),
        compiler_params=pltpu.CompilerParams(
            collective_id=0, has_side_effects=True, vmem_limit_bytes=46 * 1024 * 1024),
        name="front",
    )(x, g, w)


def dw_kernel(x_ref, g_ref, out_ref, out_buf, out_sem):
    slots, rows = out_buf.shape[0], out_buf.shape[1]
    steps = x_ref.shape[1] // rows

    def put(i):
        return pltpu.make_async_copy(
            out_buf.at[lax.rem(i, slots)], out_ref.at[pl.ds(pl.multiple_of(i * rows, rows), rows)],
            out_sem.at[lax.rem(i, slots)])

    def step(i, carry):
        @pl.when(i >= slots)
        def _():
            put(i - slots).wait()

        out_buf[lax.rem(i, slots)] = lax.dot_general(
            x_ref[:, pl.ds(pl.multiple_of(i * rows, rows), rows)], g_ref[...],
            (((0,), (0,)), ((), ())), preferred_element_type=jnp.float32)
        put(i).start()
        return carry

    lax.fori_loop(0, steps, step, 0)
    for i in range(steps - slots, steps):
        put(i).wait()


def dw(x, g, rows=128, slots=8):
    tokens, hidden = x.shape
    ffn = g.shape[1]
    return pl.pallas_call(
        dw_kernel,
        out_shape=jax.ShapeDtypeStruct((hidden, ffn), jnp.float32),
        in_specs=[pl.BlockSpec(memory_space=pltpu.VMEM)] * 2,
        out_specs=pl.BlockSpec(memory_space=pl.ANY),
        scratch_shapes=[
            pltpu.VMEM((slots, rows, ffn), jnp.float32),
            pltpu.SemaphoreType.DMA((slots,)),
        ],
        cost_estimate=pl.CostEstimate(
            flops=2 * tokens * hidden * ffn, bytes_accessed=4 * hidden * ffn, transcendentals=0),
        compiler_params=pltpu.CompilerParams(vmem_limit_bytes=40 * 1024 * 1024),
        name="dw",
    )(x, g)


def solution(mesh):
    def per_device(x, w, g):
        x = pltpu.with_memory_space_constraint(x, pltpu.HBM)
        near, far, early, x_all, g_all = front(x, g, w)
        arrived = lax.ppermute(far, "tp", CROSS)
        grad_w = dw(x_all, g_all)
        arrived = jnp.concatenate([early, arrived], axis=1)
        return (near + arrived).astype(jnp.bfloat16), grad_w

    return jax.shard_map(
        per_device,
        mesh=mesh,
        in_specs=(P(("dp", "tp"), None), P(None, "tp"), P("dp", "tp")),
        out_specs=(P(("dp", "tp"), None), P("dp", "tp")),
        check_vma=False,
    )
```

```python
import jax
import jax.numpy as jnp
from jax import lax
from jax.experimental import pallas as pl
from jax.experimental.pallas import tpu as pltpu
from jax.sharding import PartitionSpec as P


MESH = pl.DeviceIdType.MESH
CROSS = [(0, 2), (1, 3), (2, 0), (3, 1)]
CHUNK = 512
SLOTS = 4
PIECES = 4
EARLY = 384


def neighbours():
    me = lax.axis_index("tp")
    sib = me + 1 - 2 * lax.rem(me, 2)
    return me, lax.rem(me + 2, 4), sib, lax.rem(sib + 2, 4)


def front_kernel(x_ref, g_ref, w_ref, near_ref, far_ref, early_ref, x_all, g_all,
                 w_buf, own, send, recv, early_src,
                 x_sem, g_sem, w_sem, sum_send, sum_recv, sib_send, sib_recv,
                 cross_send, cross_recv, last_send, last_recv, early_send, early_recv):
    order = neighbours()
    _, cross, sib, _ = order
    tokens = x_ref.shape[0]
    chunks = w_ref.shape[0] // CHUNK
    piece = x_ref.shape[1] // PIECES

    def remote(src, dst, send_sem, recv_sem, to):
        return pltpu.make_async_remote_copy(
            src_ref=src, dst_ref=dst, send_sem=send_sem, recv_sem=recv_sem,
            device_id={"tp": to}, device_id_type=MESH)

    def block(j):
        return pl.ds(j * tokens, tokens)

    def chunk_of(c):
        return pl.ds(pl.multiple_of(c * CHUNK, CHUNK), CHUNK)

    fetch_x = pltpu.make_async_copy(x_ref, x_all.at[block(0)], x_sem)
    fetch_g = [
        pltpu.make_async_copy(
            g_ref.at[pl.ds(pl.multiple_of(idx * tokens, tokens), tokens)], g_all.at[block(j)], g_sem.at[j])
        for j, idx in enumerate(order)]

    def fetch_w(c):
        slot = lax.rem(c, SLOTS)
        return pltpu.make_async_copy(w_ref.at[chunk_of(c)], w_buf.at[slot], w_sem.at[slot])

    def cross_piece(p, src=x_ref):
        cols = pl.ds(p * piece, piece)
        return remote(src.at[:, cols], x_all.at[block(1), cols], cross_send.at[p], cross_recv.at[p], cross)

    def last_piece(p):
        cols = pl.ds(p * piece, piece)
        return remote(x_all.at[block(1), cols], x_all.at[block(3), cols], last_send.at[p], last_recv.at[p], sib)

    def to_sibling(c):
        return remote(send.at[c], recv.at[c], sum_send.at[c], sum_recv.at[c], sib)

    early = remote(early_src, early_ref, early_send, early_recv, cross)

    def x_to_sibling(src=x_ref):
        return remote(src, x_all.at[block(2)], sib_send, sib_recv, sib)

    def send_x(src):
        for p in range(PIECES):
            cross_piece(p, src).start()
        x_to_sibling(src).start()

    def first_reads():
        for copy in fetch_g:
            copy.start()
        fetch_w(0).start()

    upper = order[0] >= 2

    @pl.when(jnp.logical_not(upper))
    def _():
        fetch_x.start()
        first_reads()

    barrier = pltpu.get_barrier_semaphore()
    for to in (sib, cross):
        pl.semaphore_signal(barrier, inc=1, device_id={"tp": to}, device_id_type=MESH)
    pl.semaphore_wait(barrier, 2)

    @pl.when(jnp.logical_not(upper))
    def _():
        fetch_x.wait()
        send_x(x_all.at[block(0)])

    @pl.when(upper)
    def _():
        send_x(x_ref)
        first_reads()
        fetch_x.start()

    for c in range(1, SLOTS - 1):
        fetch_w(c).start()
    for copy in fetch_g:
        copy.wait()

    def forward(p):
        cross_piece(p).wait_recv()
        last_piece(p).start()

    def finish(c):
        to_sibling(c).wait_recv()
        near_ref[:, chunk_of(c)] = own[c, :tokens] + recv[c, :tokens]
        total = own[c, tokens:] + recv[c, tokens:]

        @pl.when(c == 0)
        def _():
            early_src[...] = total[:, :EARLY]
            far_ref[:, :CHUNK - EARLY] = total[:, EARLY:]

        @pl.when(c >= 1)
        def _():
            far_ref[:, pl.ds(pl.multiple_of(c * CHUNK - EARLY, 128), CHUNK)] = total

    def step(c, carry):
        fetch_w(c).wait()

        @pl.when(c + SLOTS - 1 < chunks)
        def _():
            fetch_w(c + SLOTS - 1).start()

        part = lax.dot_general(g_all[...], w_buf[lax.rem(c, SLOTS)], (((1,), (1,)), ((), ())),
                               preferred_element_type=jnp.float32)
        own[c] = part[:2 * tokens]
        send[c] = part[2 * tokens:]

        @pl.when(c >= 2)
        def _():
            finish(c - 2)

        to_sibling(c).start()
        for p, when in enumerate((2, 4, 6, 7)):
            @pl.when(c == when)
            def _():
                forward(p)

        @pl.when(c == 3)
        def _():
            early.start()

        return carry

    lax.fori_loop(0, chunks, step, 0)
    finish(chunks - 2)
    finish(chunks - 1)
    x_to_sibling().wait()

    @pl.when(upper)
    def _():
        fetch_x.wait()

    for c in range(chunks):
        to_sibling(c).wait_send()
    early.wait()
    for p in range(PIECES):
        cross_piece(p).wait_send()
        last_piece(p).wait()


def front(x, g, w):
    tokens, (hidden, ffn) = x.shape[0], w.shape
    chunks = hidden // CHUNK
    dma = pltpu.SemaphoreType.DMA
    sums = pltpu.VMEM((chunks, 2 * tokens, CHUNK), jnp.float32)
    return pl.pallas_call(
        front_kernel,
        out_shape=(
            jax.ShapeDtypeStruct((tokens, hidden), jnp.float32),
            jax.ShapeDtypeStruct((tokens, hidden - EARLY), jnp.float32),
            jax.ShapeDtypeStruct((tokens, EARLY), jnp.float32),
            jax.ShapeDtypeStruct((4 * tokens, hidden), x.dtype),
            jax.ShapeDtypeStruct(g.shape, g.dtype),
        ),
        in_specs=[pl.BlockSpec(memory_space=pl.ANY)] * 3,
        out_specs=[pl.BlockSpec(memory_space=pltpu.VMEM)] * 5,
        scratch_shapes=[
            pltpu.VMEM((SLOTS, CHUNK, ffn), w.dtype),
            sums, sums, sums,
            pltpu.VMEM((tokens, EARLY), jnp.float32),
            dma, dma((4,)), dma((SLOTS,)), dma((chunks,)), dma((chunks,)), dma, dma,
            dma((PIECES,)), dma((PIECES,)), dma((PIECES,)), dma((PIECES,)), dma, dma,
        ],
        cost_estimate=pl.CostEstimate(
            flops=2 * g.shape[0] * hidden * ffn, bytes_accessed=2 * hidden * ffn, transcendentals=0),
        compiler_params=pltpu.CompilerParams(
            collective_id=0, has_side_effects=True, vmem_limit_bytes=46 * 1024 * 1024),
        name="front",
    )(x, g, w)


def dw_kernel(x_ref, g_ref, out_ref, out_buf, out_sem):
    slots, rows = out_buf.shape[0], out_buf.shape[1]
    steps = x_ref.shape[1] // rows

    def put(i):
        return pltpu.make_async_copy(
            out_buf.at[lax.rem(i, slots)], out_ref.at[pl.ds(pl.multiple_of(i * rows, rows), rows)],
            out_sem.at[lax.rem(i, slots)])

    def step(i, carry):
        @pl.when(i >= slots)
        def _():
            put(i - slots).wait()

        out_buf[lax.rem(i, slots)] = lax.dot_general(
            x_ref[:, pl.ds(pl.multiple_of(i * rows, rows), rows)], g_ref[...],
            (((0,), (0,)), ((), ())), preferred_element_type=jnp.float32)
        put(i).start()
        return carry

    lax.fori_loop(0, steps, step, 0)
    for i in range(steps - slots, steps):
        put(i).wait()


def dw(x, g, rows=128, slots=8):
    tokens, hidden = x.shape
    ffn = g.shape[1]
    return pl.pallas_call(
        dw_kernel,
        out_shape=jax.ShapeDtypeStruct((hidden, ffn), jnp.float32),
        in_specs=[pl.BlockSpec(memory_space=pltpu.VMEM)] * 2,
        out_specs=pl.BlockSpec(memory_space=pl.ANY),
        scratch_shapes=[
            pltpu.VMEM((slots, rows, ffn), jnp.float32),
            pltpu.SemaphoreType.DMA((slots,)),
        ],
        cost_estimate=pl.CostEstimate(
            flops=2 * tokens * hidden * ffn, bytes_accessed=4 * hidden * ffn, transcendentals=0),
        compiler_params=pltpu.CompilerParams(vmem_limit_bytes=40 * 1024 * 1024),
        name="dw",
    )(x, g)


def solution(mesh):
    def per_device(x, w, g):
        x = pltpu.with_memory_space_constraint(x, pltpu.HBM)
        near, far, early, x_all, g_all = front(x, g, w)
        arrived = lax.ppermute(far, "tp", CROSS)
        grad_w = dw(x_all, g_all)
        arrived = jnp.concatenate([early, arrived], axis=1)
        return (near + arrived).astype(jnp.bfloat16), grad_w

    return jax.shard_map(
        per_device,
        mesh=mesh,
        in_specs=(P(("dp", "tp"), None), P(None, "tp"), P("dp", "tp")),
        out_specs=(P(("dp", "tp"), None), P("dp", "tp")),
        check_vma=False,
    )
```

```python
import jax
import jax.numpy as jnp
from jax import lax
from jax.experimental import pallas as pl
from jax.experimental.pallas import tpu as pltpu
from jax.sharding import PartitionSpec as P


MESH = pl.DeviceIdType.MESH
CROSS = [(0, 2), (1, 3), (2, 0), (3, 1)]
CHUNK = 512
SLOTS = 3
PIECES = 4
EARLY = 384


def neighbours():
    me = lax.axis_index("tp")
    sib = me + 1 - 2 * lax.rem(me, 2)
    return me, lax.rem(me + 2, 4), sib, lax.rem(sib + 2, 4)


def front_kernel(x_ref, g_ref, w_ref, near_ref, far_ref, early_ref, x_all, g_all,
                 w_buf, own, send, recv, early_src,
                 x_sem, g_sem, w_sem, sum_send, sum_recv, sib_send, sib_recv,
                 cross_send, cross_recv, last_send, last_recv, early_send, early_recv):
    order = neighbours()
    _, cross, sib, _ = order
    tokens = x_ref.shape[0]
    chunks = w_ref.shape[0] // CHUNK
    piece = x_ref.shape[1] // PIECES

    def remote(src, dst, send_sem, recv_sem, to):
        return pltpu.make_async_remote_copy(
            src_ref=src, dst_ref=dst, send_sem=send_sem, recv_sem=recv_sem,
            device_id={"tp": to}, device_id_type=MESH)

    def block(j):
        return pl.ds(j * tokens, tokens)

    def chunk_of(c):
        return pl.ds(pl.multiple_of(c * CHUNK, CHUNK), CHUNK)

    fetch_x = pltpu.make_async_copy(x_ref, x_all.at[block(0)], x_sem)
    fetch_g = [
        pltpu.make_async_copy(
            g_ref.at[pl.ds(pl.multiple_of(idx * tokens, tokens), tokens)], g_all.at[block(j)], g_sem.at[j])
        for j, idx in enumerate(order)]

    def fetch_w(c):
        slot = lax.rem(c, SLOTS)
        return pltpu.make_async_copy(w_ref.at[chunk_of(c)], w_buf.at[slot], w_sem.at[slot])

    def cross_piece(p, src=x_ref):
        cols = pl.ds(p * piece, piece)
        return remote(src.at[:, cols], x_all.at[block(1), cols], cross_send.at[p], cross_recv.at[p], cross)

    def last_piece(p):
        cols = pl.ds(p * piece, piece)
        return remote(x_all.at[block(1), cols], x_all.at[block(3), cols], last_send.at[p], last_recv.at[p], sib)

    def to_sibling(c):
        return remote(send.at[c], recv.at[c], sum_send.at[c], sum_recv.at[c], sib)

    early = remote(early_src, early_ref, early_send, early_recv, cross)

    def x_to_sibling(src=x_ref):
        return remote(src, x_all.at[block(2)], sib_send, sib_recv, sib)

    def send_x(src):
        for p in range(PIECES):
            cross_piece(p, src).start()
        x_to_sibling(src).start()

    def first_reads():
        for copy in fetch_g:
            copy.start()
        fetch_w(0).start()

    upper = order[0] >= 2

    @pl.when(jnp.logical_not(upper))
    def _():
        fetch_x.start()
        first_reads()

    barrier = pltpu.get_barrier_semaphore()
    for to in (sib, cross):
        pl.semaphore_signal(barrier, inc=1, device_id={"tp": to}, device_id_type=MESH)
    pl.semaphore_wait(barrier, 2)

    @pl.when(jnp.logical_not(upper))
    def _():
        fetch_x.wait()
        send_x(x_all.at[block(0)])

    @pl.when(upper)
    def _():
        send_x(x_ref)
        first_reads()
        fetch_x.start()

    fetch_w(1).start()
    for copy in fetch_g:
        copy.wait()

    def forward(p):
        cross_piece(p).wait_recv()
        last_piece(p).start()

    def finish(c):
        to_sibling(c).wait_recv()
        near_ref[:, chunk_of(c)] = own[c, :tokens] + recv[c, :tokens]
        total = own[c, tokens:] + recv[c, tokens:]

        @pl.when(c == 0)
        def _():
            early_src[...] = total[:, :EARLY]
            far_ref[:, :CHUNK - EARLY] = total[:, EARLY:]

        @pl.when(c >= 1)
        def _():
            far_ref[:, pl.ds(pl.multiple_of(c * CHUNK - EARLY, 128), CHUNK)] = total

    def step(c, carry):
        fetch_w(c).wait()

        @pl.when(c + 2 < chunks)
        def _():
            fetch_w(c + 2).start()

        part = lax.dot_general(g_all[...], w_buf[lax.rem(c, SLOTS)], (((1,), (1,)), ((), ())),
                               preferred_element_type=jnp.float32)
        own[c] = part[:2 * tokens]
        send[c] = part[2 * tokens:]

        @pl.when(c >= 1)
        def _():
            finish(c - 1)

        to_sibling(c).start()
        for p, when in enumerate((2, 4, 6, 7)):
            @pl.when(c == when)
            def _():
                forward(p)

        @pl.when(c == 2)
        def _():
            early.start()

        return carry

    lax.fori_loop(0, chunks, step, 0)
    finish(chunks - 1)
    x_to_sibling().wait()

    @pl.when(upper)
    def _():
        fetch_x.wait()

    for c in range(chunks):
        to_sibling(c).wait_send()
    for p in range(PIECES):
        cross_piece(p).wait_send()
        last_piece(p).wait()
    early.wait()


def front(x, g, w):
    tokens, (hidden, ffn) = x.shape[0], w.shape
    chunks = hidden // CHUNK
    dma = pltpu.SemaphoreType.DMA
    sums = pltpu.VMEM((chunks, 2 * tokens, CHUNK), jnp.float32)
    return pl.pallas_call(
        front_kernel,
        out_shape=(
            jax.ShapeDtypeStruct((tokens, hidden), jnp.float32),
            jax.ShapeDtypeStruct((tokens, hidden - EARLY), jnp.float32),
            jax.ShapeDtypeStruct((tokens, EARLY), jnp.float32),
            jax.ShapeDtypeStruct((4 * tokens, hidden), x.dtype),
            jax.ShapeDtypeStruct(g.shape, g.dtype),
        ),
        in_specs=[pl.BlockSpec(memory_space=pl.ANY)] * 3,
        out_specs=[pl.BlockSpec(memory_space=pltpu.VMEM)] * 5,
        scratch_shapes=[
            pltpu.VMEM((SLOTS, CHUNK, ffn), w.dtype),
            sums, sums, sums,
            pltpu.VMEM((tokens, EARLY), jnp.float32),
            dma, dma((4,)), dma((SLOTS,)), dma((chunks,)), dma((chunks,)), dma, dma,
            dma((PIECES,)), dma((PIECES,)), dma((PIECES,)), dma((PIECES,)), dma, dma,
        ],
        cost_estimate=pl.CostEstimate(
            flops=2 * g.shape[0] * hidden * ffn, bytes_accessed=2 * hidden * ffn, transcendentals=0),
        compiler_params=pltpu.CompilerParams(
            collective_id=0, has_side_effects=True, vmem_limit_bytes=46 * 1024 * 1024),
        name="front",
    )(x, g, w)


def dw_kernel(x_ref, g_ref, out_ref, out_buf, out_sem):
    slots, rows = out_buf.shape[0], out_buf.shape[1]
    steps = x_ref.shape[1] // rows

    def put(i):
        return pltpu.make_async_copy(
            out_buf.at[lax.rem(i, slots)], out_ref.at[pl.ds(pl.multiple_of(i * rows, rows), rows)],
            out_sem.at[lax.rem(i, slots)])

    def step(i, carry):
        @pl.when(i >= slots)
        def _():
            put(i - slots).wait()

        out_buf[lax.rem(i, slots)] = lax.dot_general(
            x_ref[:, pl.ds(pl.multiple_of(i * rows, rows), rows)], g_ref[...],
            (((0,), (0,)), ((), ())), preferred_element_type=jnp.float32)
        put(i).start()
        return carry

    lax.fori_loop(0, steps, step, 0)
    for i in range(steps - slots, steps):
        put(i).wait()


def dw(x, g, rows=128, slots=8):
    tokens, hidden = x.shape
    ffn = g.shape[1]
    return pl.pallas_call(
        dw_kernel,
        out_shape=jax.ShapeDtypeStruct((hidden, ffn), jnp.float32),
        in_specs=[pl.BlockSpec(memory_space=pltpu.VMEM)] * 2,
        out_specs=pl.BlockSpec(memory_space=pl.ANY),
        scratch_shapes=[
            pltpu.VMEM((slots, rows, ffn), jnp.float32),
            pltpu.SemaphoreType.DMA((slots,)),
        ],
        cost_estimate=pl.CostEstimate(
            flops=2 * tokens * hidden * ffn, bytes_accessed=4 * hidden * ffn, transcendentals=0),
        compiler_params=pltpu.CompilerParams(vmem_limit_bytes=40 * 1024 * 1024),
        name="dw",
    )(x, g)


def solution(mesh):
    def per_device(x, w, g):
        x = pltpu.with_memory_space_constraint(x, pltpu.HBM)
        near, far, early, x_all, g_all = front(x, g, w)
        arrived = lax.ppermute(far, "tp", CROSS)
        grad_w = dw(x_all, g_all)
        arrived = jnp.concatenate([early, arrived], axis=1)
        return (near + arrived).astype(jnp.bfloat16), grad_w

    return jax.shard_map(
        per_device,
        mesh=mesh,
        in_specs=(P(("dp", "tp"), None), P(None, "tp"), P("dp", "tp")),
        out_specs=(P(("dp", "tp"), None), P("dp", "tp")),
        check_vma=False,
    )
```
